512 devices in a mesh: sector: 16 (over y, x_hi, core), member: 32 (over x_lo, z).
Axes of the slice: x: 4 (x_hi: 2, x_lo: 2; x = x_hi * 2 + x_lo), y: 4, z: 16, core: 2. Of those that a mesh axis runs over, the one named last changes fastest.
Arguments:
- state: bfloat16 [64, 4096, 256], P('member', 'sector'), may hold values from -18 to 18
- window_mask: int32 [4096, 256], P('sector'), may hold values 0 or 1
- window_index: int32 [4096], replicated, may hold values from 0 to 31, never falling along the last dimension, each value on 1 to 256 neighbouring positions
- w_space_qkv: bfloat16 [256, 768], replicated, may hold values from -0.375 to 0.375
- w_space_out: bfloat16 [256, 256], replicated, may hold values from -0.375 to 0.375
- temp_space: float32 [8], replicated, may hold values from 0.5 to 64
- w_ens_qkv: bfloat16 [256, 768], replicated, may hold values from -0.375 to 0.375
- w_ens_out: bfloat16 [256, 256], replicated, may hold values from -0.375 to 0.375
- temp_ens: float32 [8], replicated, may hold values from 0.5 to 64
- w_in: bfloat16 [256, 1024], replicated, may hold values from -0.375 to 0.375
- w_out: bfloat16 [1024, 256], replicated, may hold values from -0.1875 to 0.1875
Outputs:
- out_state: bfloat16 [64, 4096, 256], P('member', 'sector')
The draws below stay inside these ranges and needn't reach their ends.
Inputs may be any that keep to these rules, and one draw needn't show every extreme that they name: `window_index`: window numbers never fall along the patches; a window spans 1 to 256 patches.
All inputs are finite; a program needn't handle non-finite values. No bound on the sum of `window_mask` on one device may be relied on, other than what follows from the above.
Results may differ from the reference program's by a relative error of at most 0.015.
The reference program's roundings to bfloat16 on the way count: a program that leaves them out, or rounds other values in their place, can miss the bound.
Values may be sent and summed in bfloat16 or wider, within the bound.
A program may use at most 64 MiB of HBM per device.

```python
import math
import jax
import jax.numpy as jnp
import numpy as np
from jax import lax

D = 256
H = 8
FF = 1024
RAD = 128
TOK_DEV = 256
MEMBERS = 64
PATCHES = 4096


def draw_state(key, part):
    first, second = jax.random.split(jax.random.fold_in(key, 3))
    entries = jnp.clip(jax.random.normal(first, (MEMBERS, PATCHES, D), jnp.float32), -6.0, 6.0)
    scales = jnp.exp(jax.random.uniform(second, (MEMBERS, PATCHES, 1), jnp.float32, math.log(0.3), math.log(3.0)))
    return (entries * scales).astype(jnp.bfloat16)


def draw_sampling_heat(key, random_seed_offset):
    folded = jax.random.fold_in(key, random_seed_offset)
    lower, upper = (0.5, 2.0)
    return jnp.exp(jax.random.uniform(folded, (H,), jnp.float32, math.log(lower), math.log(upper)))


def draw_temp_space(key, part):
    return draw_sampling_heat(key, 11)


def draw_temp_ens(key, part):
    return draw_sampling_heat(key, 12)


def place_ends(array, own_key, smallest, high):
    longest = array.shape.index(max(array.shape))
    spots = []
    for shift in (0, 1):
        where = [jax.random.randint(jax.random.fold_in(own_key, axis), (), 0, length) for axis, length in enumerate(array.shape)]
        where[longest] = (where[longest] + shift) % array.shape[longest]
        spots.append(tuple(where))
    return array.at[spots[0]].set(smallest).at[spots[1]].set(high)


def split_up(count, total, bound, slope):
    loads = [(1 << 20) // math.isqrt(grade ** slope) + 1 for grade in range(2, count + 1)]
    surplus, given = total - bound - (count - 1), [1] * (count - 1)
    while surplus > 0:
        free = [i for i in range(count - 1) if given[i] < bound]
        pool, budget = sum([loads[i] for i in free]), surplus
        for i in free:
            more = min(bound - given[i], max(1, budget * loads[i] // pool), surplus)
            given[i] = given[i] + more
            surplus = surplus - more
    return np.array([bound] + given)


def uneven(key, number_of, total, limit, slope):
    if number_of == 2:
        one = jax.random.randint(key, (), max(1, total - limit), min(limit, total - 1) + 1)
        return jnp.stack([one, total - one])
    sizes = jnp.asarray(split_up(number_of, total, limit, slope), jnp.int32)
    pairs = (number_of - 1) // 2
    source_of, receiver = sizes[1:1 + 2 * pairs:2], sizes[2:2 + 2 * pairs:2]
    margin = jnp.minimum(source_of - 1, limit - receiver)
    shifted = jax.random.randint(jax.random.fold_in(key, 1), (pairs,), 0, 1 << 20) % (margin + 1)
    sizes = sizes.at[1:1 + 2 * pairs:2].set(source_of - shifted).at[2:2 + 2 * pairs:2].set(receiver + shifted)
    return sizes[jax.random.permutation(jax.random.fold_in(key, 2), number_of)]


def scatter_about(own_key, dims, spread, bound, kind=jnp.bfloat16):
    drawn = jax.random.normal(own_key, dims, jnp.float32) * spread
    return jnp.minimum(jnp.maximum(drawn, -bound), bound).astype(kind)


def setup_inputs(seed: int = 0) -> dict:
    key_of = jax.random.split(jax.random.key(seed), 12)
    state = draw_state(jax.random.fold_in(key_of[11], 71), 0)
    window_mask = place_ends((jax.random.randint(key_of[1], (PATCHES, 2 * RAD), 0, 2) < 1).astype(jnp.int32), jax.random.fold_in(key_of[1], 1), 0, 1)
    window_index = jnp.searchsorted(jnp.cumsum(uneven(key_of[2], PATCHES // RAD, PATCHES, 2 * RAD, 0)), jnp.arange(PATCHES), side="right").astype(jnp.int32)
    w_space_qkv = scatter_about(key_of[3], (D, 3 * D), D ** -0.5, 0.375)
    w_space_out = scatter_about(key_of[4], (D, D), D ** -0.5, 0.375)
    temp_space = draw_temp_space(jax.random.fold_in(key_of[11], 71), 0)
    w_ens_qkv = scatter_about(key_of[6], (D, 3 * D), D ** -0.5, 0.375)
    w_ens_out = scatter_about(key_of[7], (D, D), D ** -0.5, 0.375)
    temp_ens = draw_temp_ens(jax.random.fold_in(key_of[11], 71), 0)
    w_in = scatter_about(key_of[9], (D, FF), D ** -0.5, 0.375)
    w_out = scatter_about(key_of[10], (FF, D), FF ** -0.5, 0.1875)
    return {"state": state, "window_mask": window_mask, "window_index": window_index, "w_space_qkv": w_space_qkv, "w_space_out": w_space_out, "temp_space": temp_space, "w_ens_qkv": w_ens_qkv, "w_ens_out": w_ens_out, "temp_ens": temp_ens, "w_in": w_in, "w_out": w_out}


def rms_rows(values):
    squares = lax.optimization_barrier(jnp.mean(values * values, axis=-1, keepdims=True))
    return values * lax.rsqrt(squares + 1e-06)

def head_norm(values, total_heads):
    shaped = values.reshape(values.shape[:-1] + (total_heads, values.shape[-1] // total_heads))
    squares = lax.optimization_barrier(jnp.mean(shaped * shaped, axis=-1, keepdims=True))
    return (shaped * lax.rsqrt(squares + 0.1)).reshape(values.shape)

def skew_band(table, span_width):
    row_count, columns = table.shape
    padded = jnp.pad(table, ((0, 0), (0, span_width + 1 - columns)))
    return padded.reshape(-1)[:row_count * span_width].reshape(row_count, span_width)

def attend_window(queries, keys, values, query_window, key_window, mask_rows, logit_scale):
    span_width = keys.shape[1]
    banded = skew_band(mask_rows + 1, span_width)
    same_window = query_window[:, None] == key_window[None, :]
    allowed = (banded == 2) | (banded == 1) & same_window
    scores = jnp.einsum('mqhd,mkhd->mhqk', queries.astype(jnp.float32), keys.astype(jnp.float32))
    scores = scores * logit_scale[None, :, None, None]
    scores = jnp.where(allowed[None, None], scores, -1e+30)
    row_max = lax.optimization_barrier(jnp.max(scores, axis=-1, keepdims=True))
    exponent = jnp.exp(scores - row_max)
    weights = (exponent / lax.optimization_barrier(jnp.sum(exponent, axis=-1, keepdims=True))).astype(jnp.bfloat16)
    return jnp.einsum('mhqk,mkhd->mqhd', weights.astype(jnp.float32), values.astype(jnp.float32))

def member_attention_step(row_tile_size, query_key_value_weight, output_projection_weight, sampling_heat, total_heads):
    everyone, patch_count, features = row_tile_size.shape
    head_width = features // total_heads
    normed = rms_rows(row_tile_size.astype(jnp.float32)).astype(jnp.bfloat16)
    projected = jnp.dot(normed.reshape(-1, features), query_key_value_weight, preferred_element_type=jnp.float32)
    projected = projected.reshape(everyone, patch_count, 3 * features)
    shape_heads = (everyone, patch_count, total_heads, head_width)
    query_rows = head_norm(projected[..., :features], total_heads).astype(jnp.bfloat16).reshape(shape_heads)
    key_rows = head_norm(projected[..., features:2 * features], total_heads).astype(jnp.bfloat16).reshape(shape_heads)
    value_rows = projected[..., 2 * features:].astype(jnp.bfloat16).reshape(shape_heads)
    logit_scale = sampling_heat / math.sqrt(head_width)
    scores = jnp.einsum('mphd,nphd->phmn', query_rows.astype(jnp.float32), key_rows.astype(jnp.float32))
    scores = scores * logit_scale[None, :, None, None]
    row_max = lax.optimization_barrier(jnp.max(scores, axis=-1, keepdims=True))
    exponent = jnp.exp(scores - row_max)
    weights = (exponent / lax.optimization_barrier(jnp.sum(exponent, axis=-1, keepdims=True))).astype(jnp.bfloat16)
    mixed_heads = jnp.einsum('phmn,nphd->mphd', weights.astype(jnp.float32), value_rows.astype(jnp.float32))
    mixed_heads = mixed_heads.reshape(everyone * patch_count, features).astype(jnp.bfloat16)
    update = jnp.dot(mixed_heads, output_projection_weight, preferred_element_type=jnp.float32).reshape(row_tile_size.shape)
    return (row_tile_size.astype(jnp.float32) + update).astype(jnp.bfloat16)

def feed_forward(row_tile_size, w_in, w_out):
    features = row_tile_size.shape[-1]
    normed = rms_rows(row_tile_size.astype(jnp.float32)).astype(jnp.bfloat16).reshape(-1, features)
    hidden = jax.nn.gelu(jnp.dot(normed, w_in, preferred_element_type=jnp.float32)).astype(jnp.bfloat16)
    update = jnp.dot(hidden, w_out, preferred_element_type=jnp.float32).reshape(row_tile_size.shape)
    return (row_tile_size.astype(jnp.float32) + update).astype(jnp.bfloat16)

def reference(state, window_mask, window_index, w_space_qkv, w_space_out, temp_space, w_ens_qkv, w_ens_out, temp_ens, w_in, w_out):
    block_rows = min(TOK_DEV, 256)
    head_width = D // H
    cycle_index = jnp.concatenate([window_index[PATCHES - RAD:], window_index, window_index[:RAD]])
    logit_scale = temp_space / math.sqrt(head_width)
    offsets = jnp.arange(PATCHES // block_rows, dtype=jnp.int32) * block_rows

    def one_member(member_rows):
        normed = rms_rows(member_rows.astype(jnp.float32)).astype(jnp.bfloat16)
        projected = jnp.dot(normed, w_space_qkv, preferred_element_type=jnp.float32)
        query_rows = head_norm(projected[:, :D], H).astype(jnp.bfloat16).reshape(PATCHES, H, head_width)
        key_rows = head_norm(projected[:, D:2 * D], H).astype(jnp.bfloat16).reshape(PATCHES, H, head_width)
        value_rows = projected[:, 2 * D:].astype(jnp.bfloat16).reshape(PATCHES, H, head_width)
        key_cycle = jnp.concatenate([key_rows[PATCHES - RAD:], key_rows, key_rows[:RAD]])
        value_cycle = jnp.concatenate([value_rows[PATCHES - RAD:], value_rows, value_rows[:RAD]])

        def one_block(offset):
            queries = lax.dynamic_slice_in_dim(query_rows, offset, block_rows, 0)
            keys = lax.dynamic_slice_in_dim(key_cycle, offset, block_rows + 2 * RAD, 0)
            values = lax.dynamic_slice_in_dim(value_cycle, offset, block_rows + 2 * RAD, 0)
            query_window = lax.dynamic_slice_in_dim(window_index, offset, block_rows, 0)
            key_window = lax.dynamic_slice_in_dim(cycle_index, offset, block_rows + 2 * RAD, 0)
            mask_rows = lax.dynamic_slice_in_dim(window_mask, offset, block_rows, 0)
            return attend_window(queries[None], keys[None], values[None], query_window, key_window, mask_rows, logit_scale)[0]
        outputs = lax.map(one_block, offsets)
        mixed_heads = outputs.reshape(PATCHES, D).astype(jnp.bfloat16)
        update = jnp.dot(mixed_heads, w_space_out, preferred_element_type=jnp.float32)
        return (member_rows.astype(jnp.float32) + update).astype(jnp.bfloat16)
    state_b = lax.map(one_member, state)
    grouped = state_b.reshape(MEMBERS, PATCHES // block_rows, block_rows, D).transpose(1, 0, 2, 3)

    def one_group(row_tile_size):
        return feed_forward(member_attention_step(row_tile_size, w_ens_qkv, w_ens_out, temp_ens, H), w_in, w_out)
    outputs = lax.map(one_group, grouped)
    return outputs.transpose(1, 0, 2, 3).reshape(MEMBERS, PATCHES, D)
```

```python
import math

import jax
import jax.numpy as jnp
from jax import lax
from jax.experimental import pallas as pl
from jax.experimental.pallas import tpu as pltpu
from jax.sharding import PartitionSpec as P

F32 = jnp.float32
BF16 = jnp.bfloat16
MESH = pl.DeviceIdType.MESH
NEG = -1e30
LOG2E = 1.4426950408889634

D = 256
HEAD = 32
MEM = 2
TOK = 256
RAD = 128
CH = 2
QB = TOK // CH
KB = QB + 2 * RAD
NP = 32
NZ = 16
NS = 16
GH = 4
ROWS = NP * 8


def rms_rows(x):
    squares = jnp.sum(x * x, axis=-1, keepdims=True) * (1.0 / D)
    return x * lax.rsqrt(squares + 1e-06)


def head_norm(u, ones):
    sq = u * u
    hi = sq.astype(BF16)
    lo = (sq - hi.astype(F32)).astype(BF16)
    total = jnp.dot(hi, ones, preferred_element_type=F32) + jnp.dot(
        lo, ones, preferred_element_type=F32
    )
    return u * lax.rsqrt(total * (1.0 / HEAD) + 0.1)


def attend(q, k, v, bias, scale, ssc, psc, mxs):
    n, nk = q.shape[0], k.shape[0]
    lane = lax.broadcasted_iota(jnp.int32, (n, 128), 1) // HEAD
    halves = []
    for g in range(2):
        qg = q[:, g * 128 : (g + 1) * 128].astype(F32)
        kg = k[:, g * 128 : (g + 1) * 128]
        vg = v[:, g * 128 : (g + 1) * 128]
        stack = jnp.concatenate(
            [jnp.where(lane == h, qg, 0.0).astype(BF16) for h in range(GH)], axis=0
        )
        ssc[g, : GH * n, :nk] = lax.dot_general(
            stack, kg, (((1,), (1,)), ((), ())), preferred_element_type=F32
        )
        for h in range(GH):
            rows = slice(h * n, (h + 1) * n)
            s = ssc[g, rows, :nk] * scale[g * GH + h] + bias[...]
            mxs[g, rows] = jnp.broadcast_to(jnp.max(s, axis=-1, keepdims=True), (n, 128))
        for h in range(GH):
            rows = slice(h * n, (h + 1) * n)
            top = mxs[g, rows]
            s = ssc[g, rows, :nk] * scale[g * GH + h] + bias[...]
            e = jnp.exp2(s - jnp.concatenate([top] * (nk // 128), axis=1))
            ssc[g, rows, :nk] = e
            mxs[g, rows] = jnp.broadcast_to(jnp.sum(e, axis=-1, keepdims=True), (n, 128))
        for h in range(GH):
            rows = slice(h * n, (h + 1) * n)
            inv = 1.0 / mxs[g, rows]
            w = ssc[g, rows, :nk] * jnp.concatenate([inv] * (nk // 128), axis=1)
            psc[g, rows, :nk] = w.astype(BF16)
        r = jnp.dot(psc[g, : GH * n, :nk], vg, preferred_element_type=F32)
        o = r[:n]
        for h in range(1, GH):
            o = jnp.where(lane == h, r[h * n : (h + 1) * n], o)
        halves.append(o)
    return jnp.concatenate(halves, axis=1)


def kernel(
    state_h, mask_h, wid_h, wsq_h, wso_h, ts_s, weq_h, weo_h, te_s, wi_h, wo_h,
    out_ref,
    st, mk, wid, wsq, wso, weq, weo, wi, wo,
    halo, qa, ka, va, bias_a, bias_b, ones_s, ssc, psc, mxs, fs, fr, rs, rr,
    load_sem, halo_ssem, halo_rsem, f_ssem, f_rsem, r_ssem, r_rsem, know,
):
    s = lax.axis_index("sector")
    m = lax.axis_index("member")
    xl = m // NZ
    z = lax.rem(m, NZ)

    loads = []
    for i, (a, b) in enumerate(
        [
            (wid_h, wid),
            (mask_h, mk),
            (state_h, st),
            (wsq_h, wsq),
            (wso_h, wso),
            (weq_h, weq),
            (weo_h, weo),
            (wi_h, wi),
            (wo_h, wo),
        ]
    ):
        copy = pltpu.make_async_copy(a, b, load_sem.at[i])
        copy.start()
        loads.append(copy)

    def at(dx, dz):
        return (s, lax.rem(xl + dx, 2) * NZ + lax.rem(z + dz + NZ, NZ))

    right = (lax.rem(s + 1, NS), m)
    left = (lax.rem(s + NS - 1, NS), m)
    barrier = pltpu.get_barrier_semaphore()
    for dev in (right, left, at(0, 1), at(0, -1), at(1, 1), at(1, -1)):
        pl.semaphore_signal(barrier, 1, device_id=dev, device_id_type=MESH)

    ri = lax.broadcasted_iota(jnp.int32, (D, D), 0)
    ci = lax.broadcasted_iota(jnp.int32, (D, D), 1)
    ones_s[...] = jnp.where(ri // HEAD == ci // HEAD, 1.0, 0.0).astype(BF16)
    bias_b[...] = jnp.where(lax.rem(ri, 4) == lax.rem(ci, 4), 0.0, NEG)

    loads[0].wait()
    loads[1].wait()
    for c in range(CH):
        table = jnp.concatenate(
            [
                (mk[c * QB : (c + 1) * QB, :] + 1).astype(F32),
                jnp.zeros((QB, KB - 2 * RAD), F32),
            ],
            axis=1,
        )
        row = lax.broadcasted_iota(jnp.int32, (QB, KB), 0)
        for b in range(7):
            table = jnp.where(
                lax.rem(row // (1 << b), 2) == 1, pltpu.roll(table, 1 << b, 1), table
            )
        mine = jnp.broadcast_to(wid[pl.ds(2 * s + c, 1), :].astype(F32), (QB, 128)).T
        for t in range(KB // 128):
            theirs = wid[pl.ds(lax.rem(2 * s + 31 + c + t, 32), 1), :].astype(F32)
            part = table[:, t * 128 : (t + 1) * 128]
            ok = (part > 1.5) | ((part > 0.5) & (mine == jnp.broadcast_to(theirs, (QB, 128))))
            bias_a[c, :, t * 128 : (t + 1) * 128] = jnp.where(ok, 0.0, NEG)

    pl.semaphore_wait(barrier, 6)
    loads[2].wait()
    halos = []
    for i, dev in enumerate((right, left)):
        copy = pltpu.make_async_remote_copy(
            src_ref=st.at[:, pl.ds(RAD * (1 - i), RAD), :],
            dst_ref=halo.at[i],
            send_sem=halo_ssem.at[i],
            recv_sem=halo_rsem.at[i],
            device_id=dev,
            device_id_type=MESH,
        )
        copy.start()
        halos.append(copy)

    def tell(r):
        for dz in (1 << r, -(1 << r)):
            pl.semaphore_signal(know.at[r], 1, device_id=at(0, dz), device_id_type=MESH)

    tell(0)
    ones = ones_s[...]
    scale_a = [ts_s[h] * (LOG2E / math.sqrt(HEAD)) for h in range(8)]
    scale_b = [te_s[h] * (LOG2E / math.sqrt(HEAD)) for h in range(8)]

    loads[3].wait()
    for j in range(MEM):
        normed = rms_rows(st[j].astype(F32)).astype(BF16)
        proj = jnp.dot(normed, wsq[...], preferred_element_type=F32)
        qa[j] = head_norm(proj[:, :D], ones).astype(BF16)
        ka[j, RAD : RAD + TOK] = head_norm(proj[:, D : 2 * D], ones).astype(BF16)
        va[j, RAD : RAD + TOK] = proj[:, 2 * D :].astype(BF16)

    pl.semaphore_wait(know.at[0], 2)
    tell(1)

    def halo_keys(i):
        halos[i].wait_recv()
        rows = slice(0, RAD) if i == 0 else slice(RAD + TOK, RAD + TOK + RAD)
        for j in range(MEM):
            normed = rms_rows(halo[i, j].astype(F32)).astype(BF16)
            proj = jnp.dot(normed, wsq[:, D:], preferred_element_type=F32)
            ka[j, rows] = head_norm(proj[:, :D], ones).astype(BF16)
            va[j, rows] = proj[:, D:].astype(BF16)

    low = lax.rem(lax.broadcasted_iota(jnp.int32, (QB, D), 0), 8) < 4

    def window_chunk(c):
        after = []
        for j in range(MEM):
            q = qa[j, c * QB : (c + 1) * QB]
            keys = slice(c * QB, c * QB + KB)
            o = attend(q, ka[j, keys], va[j, keys], bias_a.at[c], scale_a, ssc, psc, mxs)
            upd = jnp.dot(o.astype(BF16), wso[...], preferred_element_type=F32)
            after.append(st[j, c * QB : (c + 1) * QB].astype(F32) + upd)
        even = jnp.where(low, after[0], pltpu.roll(after[1], 4, 0))
        odd = jnp.where(low, pltpu.roll(after[0], QB - 4, 0), after[1])
        fs[c, :, 0] = even.reshape(QB // 8, 8, D).astype(BF16)
        fs[c, :, 1] = odd.reshape(QB // 8, 8, D).astype(BF16)

    order = []
    for dz in (8, 7, -7, 6, -6, 5, -5, 4, -4, 3, -3, 2, -2, 1, -1, 0):
        for dx in (1, 0):
            if (dx, dz) != (0, 0):
                order.append((dx, dz))

    def slot(dx, dz):
        return dx * NZ + dz % NZ

    def forward(c):
        sends = []
        for dx, dz in order:
            dev = at(dx, dz)
            copy = pltpu.make_async_remote_copy(
                src_ref=fs.at[c, dev[1] // 2, lax.rem(dev[1], 2)],
                dst_ref=fr.at[c, slot(dx, dz)],
                send_sem=f_ssem.at[c],
                recv_sem=f_rsem.at[c],
                device_id=dev,
                device_id_type=MESH,
            )
            copy.start()
            sends.append(copy)
        fr[c, 0] = fs[c, m // 2, lax.rem(m, 2)]
        return sends

    def await_all(ref, sem):
        pltpu.make_async_copy(ref, ref, sem).wait()

    def member_chunk(c):
        await_all(fr.at[c, pl.ds(0, NP - 1)], f_rsem.at[c])
        x = fr[c].astype(F32).reshape(ROWS, D)
        normed = rms_rows(x).astype(BF16)
        proj = jnp.dot(normed, weq[...], preferred_element_type=F32)
        q = head_norm(proj[:, :D], ones).astype(BF16)
        k = head_norm(proj[:, D : 2 * D], ones).astype(BF16)
        v = proj[:, 2 * D :].astype(BF16)
        o = attend(q, k, v, bias_b, scale_b, ssc, psc, mxs)
        x = x + jnp.dot(o.astype(BF16), weo[...], preferred_element_type=F32)
        x = x.astype(BF16).astype(F32)
        normed = rms_rows(x).astype(BF16)
        hidden = jax.nn.gelu(jnp.dot(normed, wi[...], preferred_element_type=F32)).astype(BF16)
        x = x + jnp.dot(hidden, wo[...], preferred_element_type=F32)
        rs[c] = x.reshape(NP, 8, D).astype(BF16)

    def back(c):
        sends = []
        for dx, dz in order:
            copy = pltpu.make_async_remote_copy(
                src_ref=rs.at[c, slot(dx, -dz)],
                dst_ref=rr.at[c, m // 2, lax.rem(m, 2)],
                send_sem=r_ssem.at[c],
                recv_sem=r_rsem.at[c],
                device_id=at(dx, dz),
                device_id_type=MESH,
            )
            copy.start()
            sends.append(copy)
        rr[c, m // 2, lax.rem(m, 2)] = rs[c, 0]
        return sends

    halo_keys(0)
    pl.semaphore_wait(know.at[1], 2)
    tell(2)
    loads[4].wait()
    window_chunk(0)
    pl.semaphore_wait(know.at[2], 2)
    forward(0)
    halo_keys(1)
    window_chunk(1)
    forward(1)
    for i in range(5, 9):
        loads[i].wait()
    for c in range(CH):
        member_chunk(c)
        back(c)

    for c in range(CH):
        await_all(fr.at[c, pl.ds(0, NP - 1)], r_rsem.at[c])
        even = rr[c, :, 0].astype(F32).reshape(QB, D)
        odd = rr[c, :, 1].astype(F32).reshape(QB, D)
        rows = slice(c * QB, (c + 1) * QB)
        out_ref[0, rows] = jnp.where(low, even, pltpu.roll(odd, 4, 0)).astype(BF16)
        out_ref[1, rows] = jnp.where(low, pltpu.roll(even, QB - 4, 0), odd).astype(BF16)
    for c in range(CH):
        await_all(fr.at[c, pl.ds(0, NP - 1)], f_ssem.at[c])
        await_all(fr.at[c, pl.ds(0, NP - 1)], r_ssem.at[c])
    for copy in halos:
        copy.wait_send()


def on_device(
    state,
    window_mask,
    window_index,
    w_space_qkv,
    w_space_out,
    temp_space,
    w_ens_qkv,
    w_ens_out,
    temp_ens,
    w_in,
    w_out,
):
    hbm = pl.BlockSpec(memory_space=pl.ANY)
    smem = pl.BlockSpec(memory_space=pltpu.SMEM)
    return pl.pallas_call(
        kernel,
        out_shape=jax.ShapeDtypeStruct((MEM, TOK, D), BF16),
        in_specs=[hbm, hbm, hbm, hbm, hbm, smem, hbm, hbm, smem, hbm, hbm],
        out_specs=pl.BlockSpec(memory_space=pltpu.VMEM),
        scratch_shapes=[
            pltpu.VMEM((MEM, TOK, D), BF16),
            pltpu.VMEM((TOK, 2 * RAD), jnp.int32),
            pltpu.VMEM((32, 128), jnp.int32),
            pltpu.VMEM((D, 3 * D), BF16),
            pltpu.VMEM((D, D), BF16),
            pltpu.VMEM((D, 3 * D), BF16),
            pltpu.VMEM((D, D), BF16),
            pltpu.VMEM((D, 4 * D), BF16),
            pltpu.VMEM((4 * D, D), BF16),
            pltpu.VMEM((2, MEM, RAD, D), BF16),
            pltpu.VMEM((MEM, TOK, D), BF16),
            pltpu.VMEM((MEM, TOK + 2 * RAD, D), BF16),
            pltpu.VMEM((MEM, TOK + 2 * RAD, D), BF16),
            pltpu.VMEM((CH, QB, KB), F32),
            pltpu.VMEM((D, D), F32),
            pltpu.VMEM((D, D), BF16),
            pltpu.VMEM((2, GH * ROWS, KB), F32),
            pltpu.VMEM((2, GH * ROWS, KB), BF16),
            pltpu.VMEM((2, GH * ROWS, 128), F32),
            pltpu.VMEM((CH, NP // 2, 2, 8, D), BF16),
            pltpu.VMEM((CH, NP, 8, D), BF16),
            pltpu.VMEM((CH, NP, 8, D), BF16),
            pltpu.VMEM((CH, NP // 2, 2, 8, D), BF16),
            pltpu.SemaphoreType.DMA((9,)),
            pltpu.SemaphoreType.DMA((2,)),
            pltpu.SemaphoreType.DMA((2,)),
            pltpu.SemaphoreType.DMA((CH,)),
            pltpu.SemaphoreType.DMA((CH,)),
            pltpu.SemaphoreType.DMA((CH,)),
            pltpu.SemaphoreType.DMA((CH,)),
            pltpu.SemaphoreType.REGULAR((3,)),
        ],
        compiler_params=pltpu.CompilerParams(
            collective_id=0, has_side_effects=True, vmem_limit_bytes=48 * 1024 * 1024
        ),
        name="ensemble_block",
    )(
        state,
        window_mask,
        window_index.reshape(32, 128),
        w_space_qkv,
        w_space_out,
        temp_space,
        w_ens_qkv,
        w_ens_out,
        temp_ens,
        w_in,
        w_out,
    )


def solution(mesh):
    return jax.shard_map(
        on_device,
        mesh=mesh,
        in_specs=(P("member", "sector", None), P("sector", None)) + (P(),) * 9,
        out_specs=P("member", "sector", None),
        check_vma=False,
    )
```

```python
import math

import jax
import jax.numpy as jnp
from jax import lax
from jax.experimental import pallas as pl
from jax.experimental.pallas import tpu as pltpu
from jax.sharding import PartitionSpec as P

F32 = jnp.float32
BF16 = jnp.bfloat16
MESH = pl.DeviceIdType.MESH
NEG = -1e30
LOG2E = 1.4426950408889634

D = 256
HEAD = 32
MEM = 2
TOK = 256
RAD = 128
CH = 2
QB = TOK // CH
KB = QB + 2 * RAD
NP = 32
NZ = 16
NS = 16
GH = 4
BACK = (0,1,2,3,4,15,5,14,6,13,7,12,8,11,9,10)
ROWS = NP * 8


def rms_rows(x):
    squares = jnp.sum(x * x, axis=-1, keepdims=True) * (1.0 / D)
    return x * lax.rsqrt(squares + 1e-06)


def head_norm(u, ones):
    sq = u * u
    hi = sq.astype(BF16)
    lo = (sq - hi.astype(F32)).astype(BF16)
    total = jnp.dot(hi, ones, preferred_element_type=F32) + jnp.dot(
        lo, ones, preferred_element_type=F32
    )
    return u * lax.rsqrt(total * (1.0 / HEAD) + 0.1)


def attend(q, k, v, bias, scale, ssc, psc, mxs):
    n, nk = q.shape[0], k.shape[0]
    lane = lax.broadcasted_iota(jnp.int32, (n, 128), 1) // HEAD
    halves = []
    for g in range(2):
        qg = q[:, g * 128 : (g + 1) * 128].astype(F32)
        kg = k[:, g * 128 : (g + 1) * 128]
        vg = v[:, g * 128 : (g + 1) * 128]
        stack = jnp.concatenate(
            [jnp.where(lane == h, qg, 0.0).astype(BF16) for h in range(GH)], axis=0
        )
        ssc[g, : GH * n, :nk] = lax.dot_general(
            stack, kg, (((1,), (1,)), ((), ())), preferred_element_type=F32
        )
        for h in range(GH):
            rows = slice(h * n, (h + 1) * n)
            s = ssc[g, rows, :nk] * scale[g * GH + h] + bias[...]
            mxs[g, rows] = jnp.broadcast_to(jnp.max(s, axis=-1, keepdims=True), (n, 128))
        for h in range(GH):
            rows = slice(h * n, (h + 1) * n)
            top = mxs[g, rows]
            s = ssc[g, rows, :nk] * scale[g * GH + h] + bias[...]
            e = jnp.exp2(s - jnp.concatenate([top] * (nk // 128), axis=1))
            ssc[g, rows, :nk] = e
            mxs[g, rows] = jnp.broadcast_to(jnp.sum(e, axis=-1, keepdims=True), (n, 128))
        for h in range(GH):
            rows = slice(h * n, (h + 1) * n)
            inv = 1.0 / mxs[g, rows]
            w = ssc[g, rows, :nk] * jnp.concatenate([inv] * (nk // 128), axis=1)
            psc[g, rows, :nk] = w.astype(BF16)
        r = jnp.dot(psc[g, : GH * n, :nk], vg, preferred_element_type=F32)
        o = r[:n]
        for h in range(1, GH):
            o = jnp.where(lane == h, r[h * n : (h + 1) * n], o)
        halves.append(o)
    return jnp.concatenate(halves, axis=1)


def kernel(
    state_h, mask_h, wid_h, wsq_h, wso_h, ts_s, weq_h, weo_h, te_s, wi_h, wo_h,
    out_ref,
    st, mk, wid, wsq, wso, weq, weo, wi, wo,
    halo, qa, ka, va, bias_a, bias_b, ones_s, ssc, psc, mxs, fs, fr, rs, rr,
    load_sem, halo_ssem, halo_rsem, f_ssem, f_rsem, r_ssem, r_rsem, know,
):
    s = lax.axis_index("sector")
    m = lax.axis_index("member")
    xl = m // NZ
    z = lax.rem(m, NZ)

    loads = []
    for i, (a, b) in enumerate(
        [
            (wid_h, wid),
            (mask_h, mk),
            (state_h, st),
            (wsq_h, wsq),
            (wso_h, wso),
            (weq_h, weq),
            (weo_h, weo),
            (wi_h, wi),
            (wo_h, wo),
        ]
    ):
        copy = pltpu.make_async_copy(a, b, load_sem.at[i])
        copy.start()
        loads.append(copy)

    def at(dx, dz):
        return (s, lax.rem(xl + dx, 2) * NZ + lax.rem(z + dz + NZ, NZ))

    right = (lax.rem(s + 1, NS), m)
    left = (lax.rem(s + NS - 1, NS), m)
    barrier = pltpu.get_barrier_semaphore()
    for dev in (right, left, at(0, 1), at(0, -1), at(1, 1), at(1, -1)):
        pl.semaphore_signal(barrier, 1, device_id=dev, device_id_type=MESH)

    ri = lax.broadcasted_iota(jnp.int32, (D, D), 0)
    ci = lax.broadcasted_iota(jnp.int32, (D, D), 1)
    ones_s[...] = jnp.where(ri // HEAD == ci // HEAD, 1.0, 0.0).astype(BF16)
    bias_b[...] = jnp.where(lax.rem(ri, 4) == lax.rem(ci, 4), 0.0, NEG)

    loads[0].wait()
    loads[1].wait()
    for c in range(CH):
        table = jnp.concatenate(
            [
                (mk[c * QB : (c + 1) * QB, :] + 1).astype(F32),
                jnp.zeros((QB, KB - 2 * RAD), F32),
            ],
            axis=1,
        )
        row = lax.broadcasted_iota(jnp.int32, (QB, KB), 0)
        for b in range(7):
            table = jnp.where(
                lax.rem(row // (1 << b), 2) == 1, pltpu.roll(table, 1 << b, 1), table
            )
        mine = jnp.broadcast_to(wid[pl.ds(2 * s + c, 1), :].astype(F32), (QB, 128)).T
        for t in range(KB // 128):
            theirs = wid[pl.ds(lax.rem(2 * s + 31 + c + t, 32), 1), :].astype(F32)
            part = table[:, t * 128 : (t + 1) * 128]
            ok = (part > 1.5) | ((part > 0.5) & (mine == jnp.broadcast_to(theirs, (QB, 128))))
            bias_a[c, :, t * 128 : (t + 1) * 128] = jnp.where(ok, 0.0, NEG)

    pl.semaphore_wait(barrier, 6)
    loads[2].wait()
    halos = []
    for i, dev in enumerate((right, left)):
        copy = pltpu.make_async_remote_copy(
            src_ref=st.at[:, pl.ds(RAD * (1 - i), RAD), :],
            dst_ref=halo.at[i],
            send_sem=halo_ssem.at[i],
            recv_sem=halo_rsem.at[i],
            device_id=dev,
            device_id_type=MESH,
        )
        copy.start()
        halos.append(copy)

    def tell(r):
        for dz in (1 << r, -(1 << r)):
            pl.semaphore_signal(know.at[r], 1, device_id=at(0, dz), device_id_type=MESH)

    tell(0)
    ones = ones_s[...]
    scale_a = [ts_s[h] * (LOG2E / math.sqrt(HEAD)) for h in range(8)]
    scale_b = [te_s[h] * (LOG2E / math.sqrt(HEAD)) for h in range(8)]

    loads[3].wait()
    for j in range(MEM):
        normed = rms_rows(st[j].astype(F32)).astype(BF16)
        proj = jnp.dot(normed, wsq[...], preferred_element_type=F32)
        qa[j] = head_norm(proj[:, :D], ones).astype(BF16)
        ka[j, RAD : RAD + TOK] = head_norm(proj[:, D : 2 * D], ones).astype(BF16)
        va[j, RAD : RAD + TOK] = proj[:, 2 * D :].astype(BF16)

    pl.semaphore_wait(know.at[0], 2)
    tell(1)

    def halo_keys(i):
        halos[i].wait_recv()
        rows = slice(0, RAD) if i == 0 else slice(RAD + TOK, RAD + TOK + RAD)
        for j in range(MEM):
            normed = rms_rows(halo[i, j].astype(F32)).astype(BF16)
            proj = jnp.dot(normed, wsq[:, D:], preferred_element_type=F32)
            ka[j, rows] = head_norm(proj[:, :D], ones).astype(BF16)
            va[j, rows] = proj[:, D:].astype(BF16)

    low = lax.rem(lax.broadcasted_iota(jnp.int32, (QB, D), 0), 8) < 4

    def window_chunk(c):
        after = []
        for j in range(MEM):
            q = qa[j, c * QB : (c + 1) * QB]
            keys = slice(c * QB, c * QB + KB)
            o = attend(q, ka[j, keys], va[j, keys], bias_a.at[c], scale_a, ssc, psc, mxs)
            upd = jnp.dot(o.astype(BF16), wso[...], preferred_element_type=F32)
            after.append(st[j, c * QB : (c + 1) * QB].astype(F32) + upd)
        even = jnp.where(low, after[0], pltpu.roll(after[1], 4, 0))
        odd = jnp.where(low, pltpu.roll(after[0], QB - 4, 0), after[1])
        fs[c, :, 0] = even.reshape(QB // 8, 8, D).astype(BF16)
        fs[c, :, 1] = odd.reshape(QB // 8, 8, D).astype(BF16)

    order = []
    for dz in (8, 7, -7, 6, -6, 5, -5, 4, -4, 3, -3, 2, -2, 1, -1, 0):
        for dx in (1, 0):
            if (dx, dz) != (0, 0):
                order.append((dx, dz))

    def slot(dx, dz):
        return dx * NZ + dz % NZ

    def forward(c):
        sends = []
        for dx, dz in order:
            dev = at(dx, dz)
            copy = pltpu.make_async_remote_copy(
                src_ref=fs.at[c, dev[1] // 2, lax.rem(dev[1], 2)],
                dst_ref=fr.at[c, slot(dx, dz)],
                send_sem=f_ssem.at[c],
                recv_sem=f_rsem.at[c],
                device_id=dev,
                device_id_type=MESH,
            )
            copy.start()
            sends.append(copy)
        fr[c, 0] = fs[c, m // 2, lax.rem(m, 2)]
        return sends

    def await_all(ref, sem):
        pltpu.make_async_copy(ref, ref, sem).wait()

    def member_chunk(c):
        await_all(fr.at[c, pl.ds(0, NP - 1)], f_rsem.at[c])
        x = fr[c].astype(F32).reshape(ROWS, D)
        normed = rms_rows(x).astype(BF16)
        proj = jnp.dot(normed, weq[...], preferred_element_type=F32)
        q = head_norm(proj[:, :D], ones).astype(BF16)
        k = head_norm(proj[:, D : 2 * D], ones).astype(BF16)
        v = proj[:, 2 * D :].astype(BF16)
        o = attend(q, k, v, bias_b, scale_b, ssc, psc, mxs)
        x = x + jnp.dot(o.astype(BF16), weo[...], preferred_element_type=F32)
        x = x.astype(BF16).astype(F32)
        normed = rms_rows(x).astype(BF16)
        hidden = jax.nn.gelu(jnp.dot(normed, wi[...], preferred_element_type=F32)).astype(BF16)
        x = x + jnp.dot(hidden, wo[...], preferred_element_type=F32)
        rs[c] = x.reshape(NP, 8, D).astype(BF16)

    def back(c):
        for zd in BACK:
            for dx in (1, 0):
                there = lax.rem(xl + dx, 2) * NZ + zd

                def send():
                    pltpu.make_async_remote_copy(
                        src_ref=rs.at[c, dx * NZ + lax.rem(z - zd + NZ, NZ)],
                        dst_ref=rr.at[c, m // 2, lax.rem(m, 2)],
                        send_sem=r_ssem.at[c],
                        recv_sem=r_rsem.at[c],
                        device_id=(s, there),
                        device_id_type=MESH,
                    ).start()

                if dx == 1:
                    send()
                else:
                    pl.when(zd != z)(send)
        rr[c, m // 2, lax.rem(m, 2)] = rs[c, 0]

    halo_keys(0)
    pl.semaphore_wait(know.at[1], 2)
    tell(2)
    loads[4].wait()
    window_chunk(0)
    pl.semaphore_wait(know.at[2], 2)
    forward(0)
    halo_keys(1)
    window_chunk(1)
    forward(1)
    for i in range(5, 9):
        loads[i].wait()
    for c in range(CH):
        member_chunk(c)
        back(c)

    for c in range(CH):
        await_all(fr.at[c, pl.ds(0, NP - 1)], r_rsem.at[c])
        even = rr[c, :, 0].astype(F32).reshape(QB, D)
        odd = rr[c, :, 1].astype(F32).reshape(QB, D)
        rows = slice(c * QB, (c + 1) * QB)
        out_ref[0, rows] = jnp.where(low, even, pltpu.roll(odd, 4, 0)).astype(BF16)
        out_ref[1, rows] = jnp.where(low, pltpu.roll(even, QB - 4, 0), odd).astype(BF16)
    for c in range(CH):
        await_all(fr.at[c, pl.ds(0, NP - 1)], f_ssem.at[c])
        await_all(fr.at[c, pl.ds(0, NP - 1)], r_ssem.at[c])
    for copy in halos:
        copy.wait_send()


def on_device(
    state,
    window_mask,
    window_index,
    w_space_qkv,
    w_space_out,
    temp_space,
    w_ens_qkv,
    w_ens_out,
    temp_ens,
    w_in,
    w_out,
):
    hbm = pl.BlockSpec(memory_space=pl.ANY)
    smem = pl.BlockSpec(memory_space=pltpu.SMEM)
    return pl.pallas_call(
        kernel,
        out_shape=jax.ShapeDtypeStruct((MEM, TOK, D), BF16),
        in_specs=[hbm, hbm, hbm, hbm, hbm, smem, hbm, hbm, smem, hbm, hbm],
        out_specs=pl.BlockSpec(memory_space=pltpu.VMEM),
        scratch_shapes=[
            pltpu.VMEM((MEM, TOK, D), BF16),
            pltpu.VMEM((TOK, 2 * RAD), jnp.int32),
            pltpu.VMEM((32, 128), jnp.int32),
            pltpu.VMEM((D, 3 * D), BF16),
            pltpu.VMEM((D, D), BF16),
            pltpu.VMEM((D, 3 * D), BF16),
            pltpu.VMEM((D, D), BF16),
            pltpu.VMEM((D, 4 * D), BF16),
            pltpu.VMEM((4 * D, D), BF16),
            pltpu.VMEM((2, MEM, RAD, D), BF16),
            pltpu.VMEM((MEM, TOK, D), BF16),
            pltpu.VMEM((MEM, TOK + 2 * RAD, D), BF16),
            pltpu.VMEM((MEM, TOK + 2 * RAD, D), BF16),
            pltpu.VMEM((CH, QB, KB), F32),
            pltpu.VMEM((D, D), F32),
            pltpu.VMEM((D, D), BF16),
            pltpu.VMEM((2, GH * ROWS, KB), F32),
            pltpu.VMEM((2, GH * ROWS, KB), BF16),
            pltpu.VMEM((2, GH * ROWS, 128), F32),
            pltpu.VMEM((CH, NP // 2, 2, 8, D), BF16),
            pltpu.VMEM((CH, NP, 8, D), BF16),
            pltpu.VMEM((CH, NP, 8, D), BF16),
            pltpu.VMEM((CH, NP // 2, 2, 8, D), BF16),
            pltpu.SemaphoreType.DMA((9,)),
            pltpu.SemaphoreType.DMA((2,)),
            pltpu.SemaphoreType.DMA((2,)),
            pltpu.SemaphoreType.DMA((CH,)),
            pltpu.SemaphoreType.DMA((CH,)),
            pltpu.SemaphoreType.DMA((CH,)),
            pltpu.SemaphoreType.DMA((CH,)),
            pltpu.SemaphoreType.REGULAR((3,)),
        ],
        compiler_params=pltpu.CompilerParams(
            collective_id=0, has_side_effects=True, vmem_limit_bytes=67043328
        ),
        name="ensemble_block",
    )(
        state,
        window_mask,
        window_index.reshape(32, 128),
        w_space_qkv,
        w_space_out,
        temp_space,
        w_ens_qkv,
        w_ens_out,
        temp_ens,
        w_in,
        w_out,
    )


def solution(mesh):
    return jax.shard_map(
        on_device,
        mesh=mesh,
        in_specs=(P("member", "sector", None), P("sector", None)) + (P(),) * 9,
        out_specs=P("member", "sector", None),
        check_vma=False,
    )
```

```python
import math

import jax
import jax.numpy as jnp
from jax import lax
from jax.experimental import pallas as pl
from jax.experimental.pallas import tpu as pltpu
from jax.sharding import PartitionSpec as P

F32 = jnp.float32
BF16 = jnp.bfloat16
MESH = pl.DeviceIdType.MESH
NEG = -1e30
LOG2E = 1.4426950408889634

D = 256
HEAD = 32
MEM = 2
TOK = 256
RAD = 128
CH = 2
QB = TOK // CH
KB = QB + 2 * RAD
NP = 32
NZ = 16
NS = 16
GH = 4
BACK = (0, 1, 2, 3, 8, 9, 10, 11, 7, 15, 6, 14, 5, 13, 4, 12)
ROWS = NP * 8


def rms_rows(x):
    squares = jnp.sum(x * x, axis=-1, keepdims=True) * (1.0 / D)
    return x * lax.rsqrt(squares + 1e-06)


def head_norm(u, ones):
    sq = u * u
    hi = sq.astype(BF16)
    lo = (sq - hi.astype(F32)).astype(BF16)
    total = jnp.dot(hi, ones, preferred_element_type=F32) + jnp.dot(
        lo, ones, preferred_element_type=F32
    )
    return u * lax.rsqrt(total * (1.0 / HEAD) + 0.1)


def attend(q, k, v, bias, scale, ssc, psc, mxs):
    n, nk = q.shape[0], k.shape[0]
    lane = lax.broadcasted_iota(jnp.int32, (n, 128), 1) // HEAD
    halves = []
    for g in range(2):
        qg = q[:, g * 128 : (g + 1) * 128].astype(F32)
        kg = k[:, g * 128 : (g + 1) * 128]
        vg = v[:, g * 128 : (g + 1) * 128]
        stack = jnp.concatenate(
            [jnp.where(lane == h, qg, 0.0).astype(BF16) for h in range(GH)], axis=0
        )
        ssc[g, : GH * n, :nk] = lax.dot_general(
            stack, kg, (((1,), (1,)), ((), ())), preferred_element_type=F32
        )
        for h in range(GH):
            rows = slice(h * n, (h + 1) * n)
            s = ssc[g, rows, :nk] * scale[g * GH + h] + bias[...]
            mxs[g, rows] = jnp.broadcast_to(jnp.max(s, axis=-1, keepdims=True), (n, 128))
        for h in range(GH):
            rows = slice(h * n, (h + 1) * n)
            top = mxs[g, rows]
            s = ssc[g, rows, :nk] * scale[g * GH + h] + bias[...]
            e = jnp.exp2(s - jnp.concatenate([top] * (nk // 128), axis=1))
            ssc[g, rows, :nk] = e
            mxs[g, rows] = jnp.broadcast_to(jnp.sum(e, axis=-1, keepdims=True), (n, 128))
        for h in range(GH):
            rows = slice(h * n, (h + 1) * n)
            inv = 1.0 / mxs[g, rows]
            w = ssc[g, rows, :nk] * jnp.concatenate([inv] * (nk // 128), axis=1)
            psc[g, rows, :nk] = w.astype(BF16)
        r = jnp.dot(psc[g, : GH * n, :nk], vg, preferred_element_type=F32)
        o = r[:n]
        for h in range(1, GH):
            o = jnp.where(lane == h, r[h * n : (h + 1) * n], o)
        halves.append(o)
    return jnp.concatenate(halves, axis=1)


def kernel(
    state_h, mask_h, wid_h, wsq_h, wso_h, ts_h, weq_h, weo_h, te_h, wi_h, wo_h,
    out_ref,
    st, mk, wid, wsq, wso, weq, weo, wi, wo, ts_s, te_s,
    halo, qa, ka, va, bias_a, bias_b, ones_s, ssc, psc, mxs, fs, fr, rs, rr,
    load_sem, halo_ssem, halo_rsem, f_ssem, f_rsem, r_ssem, r_rsem, know,
):
    s = lax.axis_index("sector")
    m = lax.axis_index("member")
    xl = m // NZ
    z = lax.rem(m, NZ)

    loads = []
    for i, (a, b) in enumerate(
        [
            (wid_h, wid),
            (mask_h, mk),
            (state_h, st),
            (wsq_h, wsq),
            (wso_h, wso),
            (weq_h, weq),
            (weo_h, weo),
            (wi_h, wi),
            (wo_h, wo),
            (ts_h, ts_s),
            (te_h, te_s),
        ]
    ):
        copy = pltpu.make_async_copy(a, b, load_sem.at[i])
        copy.start()
        loads.append(copy)

    def at(dx, dz):
        return (s, lax.rem(xl + dx, 2) * NZ + lax.rem(z + dz + NZ, NZ))

    right = (lax.rem(s + 1, NS), m)
    left = (lax.rem(s + NS - 1, NS), m)
    barrier = pltpu.get_barrier_semaphore()
    for dev in (right, left, at(0, 1), at(0, -1), at(1, 1), at(1, -1)):
        pl.semaphore_signal(barrier, 1, device_id=dev, device_id_type=MESH)

    ri = lax.broadcasted_iota(jnp.int32, (D, D), 0)
    ci = lax.broadcasted_iota(jnp.int32, (D, D), 1)
    ones_s[...] = jnp.where(ri // HEAD == ci // HEAD, 1.0, 0.0).astype(BF16)
    bias_b[...] = jnp.where(lax.rem(ri, 4) == lax.rem(ci, 4), 0.0, NEG)

    loads[0].wait()
    loads[1].wait()
    for c in range(CH):
        table = jnp.concatenate(
            [
                (mk[c * QB : (c + 1) * QB, :] + 1).astype(F32),
                jnp.zeros((QB, KB - 2 * RAD), F32),
            ],
            axis=1,
        )
        row = lax.broadcasted_iota(jnp.int32, (QB, KB), 0)
        for b in range(7):
            table = jnp.where(
                lax.rem(row // (1 << b), 2) == 1, pltpu.roll(table, 1 << b, 1), table
            )
        mine = jnp.broadcast_to(wid[pl.ds(2 * s + c, 1), :].astype(F32), (QB, 128)).T
        for t in range(KB // 128):
            theirs = wid[pl.ds(lax.rem(2 * s + 31 + c + t, 32), 1), :].astype(F32)
            part = table[:, t * 128 : (t + 1) * 128]
            ok = (part > 1.5) | ((part > 0.5) & (mine == jnp.broadcast_to(theirs, (QB, 128))))
            bias_a[c, :, t * 128 : (t + 1) * 128] = jnp.where(ok, 0.0, NEG)

    pl.semaphore_wait(barrier, 6)
    loads[2].wait()
    halos = []
    for i, dev in enumerate((right, left)):
        copy = pltpu.make_async_remote_copy(
            src_ref=st.at[:, pl.ds(RAD * (1 - i), RAD), :],
            dst_ref=halo.at[i],
            send_sem=halo_ssem.at[i],
            recv_sem=halo_rsem.at[i],
            device_id=dev,
            device_id_type=MESH,
        )
        copy.start()
        halos.append(copy)

    def tell(r):
        for dz in (1 << r, -(1 << r)):
            pl.semaphore_signal(know.at[r], 1, device_id=at(0, dz), device_id_type=MESH)

    tell(0)
    ones = ones_s[...]
    loads[9].wait()
    loads[10].wait()
    scale_a = [ts_s[h] * (LOG2E / math.sqrt(HEAD)) for h in range(8)]
    scale_b = [te_s[h] * (LOG2E / math.sqrt(HEAD)) for h in range(8)]

    loads[3].wait()
    for j in range(MEM):
        normed = rms_rows(st[j].astype(F32)).astype(BF16)
        proj = jnp.dot(normed, wsq[...], preferred_element_type=F32)
        qa[j] = head_norm(proj[:, :D], ones).astype(BF16)
        ka[j, RAD : RAD + TOK] = head_norm(proj[:, D : 2 * D], ones).astype(BF16)
        va[j, RAD : RAD + TOK] = proj[:, 2 * D :].astype(BF16)

    pl.semaphore_wait(know.at[0], 2)
    tell(1)

    def halo_keys(i):
        halos[i].wait_recv()
        rows = slice(0, RAD) if i == 0 else slice(RAD + TOK, RAD + TOK + RAD)
        for j in range(MEM):
            normed = rms_rows(halo[i, j].astype(F32)).astype(BF16)
            proj = jnp.dot(normed, wsq[:, D:], preferred_element_type=F32)
            ka[j, rows] = head_norm(proj[:, :D], ones).astype(BF16)
            va[j, rows] = proj[:, D:].astype(BF16)

    low = lax.rem(lax.broadcasted_iota(jnp.int32, (QB, D), 0), 8) < 4

    def window_chunk(c):
        after = []
        for j in range(MEM):
            q = qa[j, c * QB : (c + 1) * QB]
            keys = slice(c * QB, c * QB + KB)
            o = attend(q, ka[j, keys], va[j, keys], bias_a.at[c], scale_a, ssc, psc, mxs)
            upd = jnp.dot(o.astype(BF16), wso[...], preferred_element_type=F32)
            after.append(st[j, c * QB : (c + 1) * QB].astype(F32) + upd)
        even = jnp.where(low, after[0], pltpu.roll(after[1], 4, 0))
        odd = jnp.where(low, pltpu.roll(after[0], QB - 4, 0), after[1])
        fs[c, :, 0] = even.reshape(QB // 8, 8, D).astype(BF16)
        fs[c, :, 1] = odd.reshape(QB // 8, 8, D).astype(BF16)

    order = []
    for dz in (8, 7, -7, 6, -6, 5, -5, 4, -4, 3, -3, 2, -2, 1, -1, 0):
        for dx in (1, 0):
            if (dx, dz) != (0, 0):
                order.append((dx, dz))

    def slot(dx, dz):
        return dx * NZ + dz % NZ

    def forward(c):
        sends = []
        for dx, dz in order:
            dev = at(dx, dz)
            copy = pltpu.make_async_remote_copy(
                src_ref=fs.at[c, dev[1] // 2, lax.rem(dev[1], 2)],
                dst_ref=fr.at[c, slot(dx, dz)],
                send_sem=f_ssem.at[c],
                recv_sem=f_rsem.at[c],
                device_id=dev,
                device_id_type=MESH,
            )
            copy.start()
            sends.append(copy)
        fr[c, 0] = fs[c, m // 2, lax.rem(m, 2)]
        return sends

    def await_all(ref, sem):
        pltpu.make_async_copy(ref, ref, sem).wait()

    def member_chunk(c):
        await_all(fr.at[c, pl.ds(0, NP - 1)], f_rsem.at[c])
        x = fr[c].astype(F32).reshape(ROWS, D)
        normed = rms_rows(x).astype(BF16)
        proj = jnp.dot(normed, weq[...], preferred_element_type=F32)
        q = head_norm(proj[:, :D], ones).astype(BF16)
        k = head_norm(proj[:, D : 2 * D], ones).astype(BF16)
        v = proj[:, 2 * D :].astype(BF16)
        o = attend(q, k, v, bias_b, scale_b, ssc, psc, mxs)
        x = x + jnp.dot(o.astype(BF16), weo[...], preferred_element_type=F32)
        x = x.astype(BF16).astype(F32)
        normed = rms_rows(x).astype(BF16)
        hidden = jax.nn.gelu(jnp.dot(normed, wi[...], preferred_element_type=F32)).astype(BF16)
        x = x + jnp.dot(hidden, wo[...], preferred_element_type=F32)
        rs[c] = x.reshape(NP, 8, D).astype(BF16)

    def back(c):
        if c < CH - 1:
            for dx, dz in order:
                pltpu.make_async_remote_copy(
                    src_ref=rs.at[c, slot(dx, -dz)],
                    dst_ref=rr.at[c, m // 2, lax.rem(m, 2)],
                    send_sem=r_ssem.at[c],
                    recv_sem=r_rsem.at[c],
                    device_id=at(dx, dz),
                    device_id_type=MESH,
                ).start()
        else:
            for zd in BACK:
                for dx in (1, 0):
                    there = lax.rem(xl + dx, 2) * NZ + zd

                    def send():
                        pltpu.make_async_remote_copy(
                            src_ref=rs.at[c, dx * NZ + lax.rem(z - zd + NZ, NZ)],
                            dst_ref=rr.at[c, m // 2, lax.rem(m, 2)],
                            send_sem=r_ssem.at[c],
                            recv_sem=r_rsem.at[c],
                            device_id=(s, there),
                            device_id_type=MESH,
                        ).start()

                    if dx == 1:
                        send()
                    else:
                        pl.when(zd != z)(send)
        rr[c, m // 2, lax.rem(m, 2)] = rs[c, 0]

    halo_keys(0)
    pl.semaphore_wait(know.at[1], 2)
    tell(2)
    loads[4].wait()
    window_chunk(0)
    pl.semaphore_wait(know.at[2], 2)
    forward(0)
    halo_keys(1)
    window_chunk(1)
    forward(1)
    for i in range(5, 9):
        loads[i].wait()
    for c in range(CH):
        member_chunk(c)
        back(c)

    for c in range(CH):
        await_all(fr.at[c, pl.ds(0, NP - 1)], r_rsem.at[c])
        even = rr[c, :, 0].astype(F32).reshape(QB, D)
        odd = rr[c, :, 1].astype(F32).reshape(QB, D)
        rows = slice(c * QB, (c + 1) * QB)
        out_ref[0, rows] = jnp.where(low, even, pltpu.roll(odd, 4, 0)).astype(BF16)
        out_ref[1, rows] = jnp.where(low, pltpu.roll(even, QB - 4, 0), odd).astype(BF16)
    for c in range(CH):
        await_all(fr.at[c, pl.ds(0, NP - 1)], f_ssem.at[c])
        await_all(fr.at[c, pl.ds(0, NP - 1)], r_ssem.at[c])
    for copy in halos:
        copy.wait_send()


def on_device(
    state,
    window_mask,
    window_index,
    w_space_qkv,
    w_space_out,
    temp_space,
    w_ens_qkv,
    w_ens_out,
    temp_ens,
    w_in,
    w_out,
):
    hbm = pl.BlockSpec(memory_space=pl.ANY)
    return pl.pallas_call(
        kernel,
        out_shape=jax.ShapeDtypeStruct((MEM, TOK, D), BF16),
        in_specs=[hbm] * 11,
        out_specs=pl.BlockSpec(memory_space=pltpu.VMEM),
        scratch_shapes=[
            pltpu.VMEM((MEM, TOK, D), BF16),
            pltpu.VMEM((TOK, 2 * RAD), jnp.int32),
            pltpu.VMEM((32, 128), jnp.int32),
            pltpu.VMEM((D, 3 * D), BF16),
            pltpu.VMEM((D, D), BF16),
            pltpu.VMEM((D, 3 * D), BF16),
            pltpu.VMEM((D, D), BF16),
            pltpu.VMEM((D, 4 * D), BF16),
            pltpu.VMEM((4 * D, D), BF16),
            pltpu.SMEM((8,), F32),
            pltpu.SMEM((8,), F32),
            pltpu.VMEM((2, MEM, RAD, D), BF16),
            pltpu.VMEM((MEM, TOK, D), BF16),
            pltpu.VMEM((MEM, TOK + 2 * RAD, D), BF16),
            pltpu.VMEM((MEM, TOK + 2 * RAD, D), BF16),
            pltpu.VMEM((CH, QB, KB), F32),
            pltpu.VMEM((D, D), F32),
            pltpu.VMEM((D, D), BF16),
            pltpu.VMEM((2, GH * ROWS, KB), F32),
            pltpu.VMEM((2, GH * ROWS, KB), BF16),
            pltpu.VMEM((2, GH * ROWS, 128), F32),
            pltpu.VMEM((CH, NP // 2, 2, 8, D), BF16),
            pltpu.VMEM((CH, NP, 8, D), BF16),
            pltpu.VMEM((CH, NP, 8, D), BF16),
            pltpu.VMEM((CH, NP // 2, 2, 8, D), BF16),
            pltpu.SemaphoreType.DMA((11,)),
            pltpu.SemaphoreType.DMA((2,)),
            pltpu.SemaphoreType.DMA((2,)),
            pltpu.SemaphoreType.DMA((CH,)),
            pltpu.SemaphoreType.DMA((CH,)),
            pltpu.SemaphoreType.DMA((CH,)),
            pltpu.SemaphoreType.DMA((CH,)),
            pltpu.SemaphoreType.REGULAR((3,)),
        ],
        compiler_params=pltpu.CompilerParams(
            collective_id=0, has_side_effects=True, vmem_limit_bytes=67043328
        ),
        name="ensemble_block",
    )(
        state,
        window_mask,
        window_index.reshape(32, 128),
        w_space_qkv,
        w_space_out,
        temp_space,
        w_ens_qkv,
        w_ens_out,
        temp_ens,
        w_in,
        w_out,
    )


def solution(mesh):
    return jax.shard_map(
        on_device,
        mesh=mesh,
        in_specs=(P("member", "sector", None), P("sector", None)) + (P(),) * 9,
        out_specs=P("member", "sector", None),
        check_vma=False,
    )
```
